256 devices in a mesh: sub: 4 (over y), dev: 64 (over x, z, core).
Axes of the slice: x: 4, y: 4, z: 8, core: 2. Of those that a mesh axis runs over, the one named last changes fastest.
Arguments:
- child_tiles: float32 [8192, 128, 128], P(('sub', 'dev')), parts along dimension 0, may hold values from -6 to 6
- l_slab: float32 [262144, 512], P(('sub', 'dev')), parts along dimension 0, may hold values from -6 to 6
- u_slab: float32 [512, 131072], P(None, ('sub', 'dev')), parts along dimension 1, may hold values from -0.25 to 0.25
- parent_own_entries: float32 [9216, 128, 128], P(('sub', 'dev')), parts along dimension 0, may hold values from -6 to 6
- parent_label: int32 [8, 32], P('sub'), parts along dimension 0, may hold values from 0 to 47, as said below
Outputs:
- parent_front: float32 [9216, 128, 128], P(('sub', 'dev')), parts along dimension 0
The draws below stay inside these ranges and needn't reach their ends.
There are 4 independent parts, one for each index of `sub`. The reference program is written for one: setup_inputs(seed, part) draws one part's arguments, and reference() takes and returns one part's arrays. A program takes and returns all parts, laid end to end along the dimension named above; each array names one. Nothing has to cross between parts.
Inputs may be any that keep to these rules, and one draw needn't show every extreme that they name: `parent_label`: the 32 labels of one child are distinct. For child c and tile row k, the label modulo 8 is sigma((k mod 8 + k // 8 + 4 c) mod 8), with sigma a permutation of 0 to 7 common to both children.
All inputs are finite; a program needn't handle non-finite values.
Results may differ from the reference program's by a relative error of at most 0.000051.
Values sent between devices are 32-bit elements; how exact they have to be, the bound alone decides.
A program may use at most 64 MiB of HBM per device.

```python
import jax
import jax.numpy as jnp
from jax import lax

TILE_EDGE = 128
MT = 32
PT = 48
PANEL = 512
CGR = 4
PR = 8
CGC = 8
PC = 8
NCD = 32
TPD = 32
PSLOTS = 36
LROWS = 1024
UCOLS = 512
N_DEV = 64


def draw_parent_label(key, part):
    result = []
    sigma = jax.random.permutation(jax.random.fold_in(key, 7), 8).astype(jnp.int32)
    for child_id in range(2):
        sub_key = jax.random.fold_in(key, 11 + child_id)
        key_score = jax.random.fold_in(sub_key, 2)
        index = jnp.arange(MT, dtype=jnp.int32)
        residue = sigma[(index % 8 + index // 8 + 4 * child_id) % 8]
        scores = jax.random.randint(key_score, (8, PT // 8), 0, 2 ** 20, dtype=jnp.int32)
        scores = scores * (PT // 8) + jnp.arange(PT // 8, dtype=jnp.int32)[None, :]
        chosen = jnp.argsort(scores, axis=1)[:, :MT // 8].astype(jnp.int32)
        quotient = chosen[residue, index // 8]
        result.append(8 * quotient + residue)
    return jnp.stack(result).astype(jnp.int32)


def level_of(stream_key, extent, split, low, largest):
    gain = 1.0
    for axis_at, blocks in split:
        heights = jax.random.uniform(jax.random.fold_in(jax.random.fold_in(stream_key, 6), axis_at), (blocks,), jnp.float32, low / len(split), largest / len(split))
        gain = gain * jnp.repeat(jnp.exp(heights), extent[axis_at] // blocks).reshape((-1,) + (1,) * (len(extent) - 1 - axis_at))
    return gain


def bell_draw(rng, shape, width, most, pieces=(), kind=jnp.bfloat16):
    values = width * jax.random.normal(rng, shape, jnp.float32)
    if pieces:
        values = values * level_of(rng, shape, pieces, -0.22, 0.18)
    return jnp.clip(values, -most, most).astype(kind)


def setup_inputs(seed: int = 0, part: int = 0) -> dict:
    keys = jax.random.split(jax.random.key(seed), 6)
    part_keys = jax.random.split(jax.random.fold_in(keys[5], part), 6)
    return {
        "child_tiles": bell_draw(part_keys[0], (N_DEV * TPD, TILE_EDGE, TILE_EDGE), 1.0, 6.0, ((0, 64),), jnp.float32),
        "l_slab": bell_draw(part_keys[1], (N_DEV * LROWS, PANEL), 1.0, 6.0, ((0, 64),), jnp.float32),
        "u_slab": bell_draw(part_keys[2], (PANEL, N_DEV * UCOLS), PANEL ** -0.5, 0.25, ((1, 64),), jnp.float32),
        "parent_own_entries": bell_draw(part_keys[3], (N_DEV * PSLOTS, TILE_EDGE, TILE_EDGE), 1.0, 6.0, ((0, 64),), jnp.float32),
        "parent_label": draw_parent_label(jax.random.fold_in(jax.random.fold_in(keys[5], part), 71), part),
    }


def reference(child_tiles, l_slab, u_slab, parent_own_entries, parent_label):
    rows_loc = MT // CGR
    cols_loc = MT // CGC
    left_parts = l_slab.reshape(N_DEV, LROWS, PANEL)
    right_parts = u_slab.reshape(PANEL, N_DEV, UCOLS).transpose(1, 0, 2)

    def device_update(pair):
        product = jnp.dot(pair[0], pair[1], precision=lax.Precision.HIGHEST, preferred_element_type=jnp.float32)
        return product.reshape(rows_loc, TILE_EDGE, cols_loc, TILE_EDGE).transpose(0, 2, 1, 3).reshape(TPD, TILE_EDGE, TILE_EDGE)

    products = lax.map(device_update, (left_parts, right_parts)).reshape(N_DEV * TPD, TILE_EDGE, TILE_EDGE)
    updated = child_tiles - products
    glob = jnp.arange(N_DEV * TPD, dtype=jnp.int32)
    device = glob // TPD
    local = glob % TPD
    child_id = device // NCD
    inner = device % NCD
    row_cls = inner // CGC
    col_cls = inner % CGC
    tile_row = row_cls + CGR * (local // cols_loc)
    tile_col = col_cls + CGC * (local % cols_loc)
    label_row = parent_label[child_id, tile_row]
    label_col = parent_label[child_id, tile_col]
    dest_dev = (label_row % PR) * PC + label_col % PC
    dest_slot = (label_row // PR) * (PT // PC) + label_col // PC
    target = (dest_dev * PSLOTS + dest_slot).astype(jnp.int32)
    return parent_own_entries + jax.ops.segment_sum(updated, target, num_segments=N_DEV * PSLOTS)
```

```python
import functools

import jax
import jax.numpy as jnp
from jax import lax
from jax.experimental import pallas as pl
from jax.experimental.pallas import tpu as pltpu
from jax.sharding import PartitionSpec as P

TILE = 128
F32 = jnp.float32
BF16 = jnp.bfloat16
MESH = pl.DeviceIdType.MESH
CHUNKS = ((0, 8), (8, 16), (24, 32), (56, 32), (88, 40))
NCH = len(CHUNKS)
OWNERS = 32
ZERO = OWNERS


def place(index):
    return index // 16, index // 2 % 8, index % 2


def offset(order):
    group = order // 4
    size = 4 - (group + 1) // 2
    step = size * (2 * (group % 2) - 1)
    return order // 2 % 2, step, order % 2


def owner(me, order):
    x, z, core = place(me)
    flip_x, step, flip_core = offset(order)
    to_x = x // 2 * 2 + (x + flip_x) % 2
    to_z = (z + step + 8) % 8
    to_core = (core + flip_core) % 2
    return to_x, to_z, to_core


def kernel(labels_hbm, child_hbm, l_hbm, u_hbm, entries_hbm, front, *scratch):
    (child, left, right, right_hi, right_lo, outgoing, packed) = scratch[:7]
    swapped = scratch[7 : 7 + NCH]
    received = scratch[7 + NCH : 7 + 2 * NCH]
    own = scratch[7 + 2 * NCH : 7 + 3 * NCH]
    labels, row_at, own_at, other_at, load_sem, swap_send, swap_recv, send_sem, recv_sem = (
        scratch[7 + 3 * NCH :]
    )
    me = lax.axis_index("dev")
    x, z, core = place(me)
    side = x // 2
    partner = me + (3 - 2 * x) * 16
    my_slot = x % 2 * 16 + z * 2 + core
    row_class = x % 2 * 2 + z // 4
    col_class = z % 4 * 2 + core

    loads = [
        pltpu.make_async_copy(source, target, load_sem.at[n])
        for n, (source, target) in enumerate(
            ((u_hbm, right), (l_hbm, left), (child_hbm, child), (entries_hbm, front), (labels_hbm, labels))
        )
    ]
    loads[4].start()
    for load in loads[:3]:
        load.start()

    barrier = pltpu.get_barrier_semaphore()
    pl.semaphore_signal(barrier, inc=1, device_id={"dev": partner}, device_id_type=MESH)

    def greet(order):
        to_x, to_z, to_core = owner(me, order)
        pl.semaphore_signal(
            barrier,
            inc=1,
            device_id={"dev": to_x * 16 + to_z * 2 + to_core},
            device_id_type=MESH,
        )

    def greet_step(order, carry):
        greet(order)
        return carry

    lax.fori_loop(0, 28, greet_step, 0)
    for order in (29, 30, 31):
        greet(order)

    loads[4].wait()
    row_classes = [labels[side, row_class + 4 * k] % 8 for k in range(8)]
    for c in range(8):
        at = jnp.int32(0)
        for k in range(1, 8):
            at = jnp.where(row_classes[k] == c, k, at)
        row_at[c] = at
    own_classes = [labels[side, col_class + 8 * m] % 8 for m in range(4)]
    other_classes = [labels[1 - side, col_class + 8 * m] % 8 for m in range(4)]
    for c in range(8):
        at = jnp.int32(-1)
        for m in range(4):
            at = jnp.where(own_classes[m] == c, m, at)
        own_at[c] = at
        at = jnp.int32(0)
        for m in range(1, 4):
            at = jnp.where(other_classes[m] == c, m, at)
        other_at[c] = at

    loads[0].wait()
    right_hi[...] = right[...].astype(BF16)
    right_lo[...] = (right[...] - right_hi[...].astype(F32)).astype(BF16)
    loads[1].wait()
    loads[2].wait()

    def update(c, put):
        k = row_at[c]
        rows = left[k]
        high = rows.astype(BF16)
        low = (rows - high.astype(F32)).astype(BF16)
        for half in range(2):
            columns = pl.ds(half * 256, 256)
            hi_columns = right_hi[:, columns]
            product = jnp.dot(high, hi_columns, preferred_element_type=F32)
            product += jnp.dot(low, hi_columns, preferred_element_type=F32)
            product += jnp.dot(high, right_lo[:, columns], preferred_element_type=F32)
            for part in range(2):
                m = 2 * half + part
                put(m, child[k * 4 + m] - product[:, part * TILE : part * TILE + TILE])

    def other_step(n, carry):
        def put(m, tile):
            outgoing[n * 4 + m] = tile

        update((1 - side) * 4 + n, put)
        return carry

    def own_step(n, carry):
        def put(m, tile):
            for part, (first, count) in zip(own, CHUNKS):
                part[n * 4 + m] = tile[first : first + count]

        update(side * 4 + n, put)
        return carry

    lax.fori_loop(0, 4, other_step, 0)
    pl.semaphore_wait(barrier, OWNERS)

    swaps = []
    for n, (first, count) in enumerate(CHUNKS):
        swaps.append(
            pltpu.make_async_remote_copy(
                src_ref=outgoing.at[:, pl.ds(first, count), :],
                dst_ref=swapped[n],
                send_sem=swap_send.at[n],
                recv_sem=swap_recv.at[n],
                device_id={"dev": partner},
                device_id_type=MESH,
            )
        )
        swaps[n].start()
    loads[3].start()
    lax.fori_loop(0, 4, own_step, 0)

    for n, (first, count) in enumerate(CHUNKS):
        rows = pl.ds(first, count)
        received[n][ZERO] = jnp.zeros((count, TILE), F32)
        swaps[n].wait_recv()

        def pick(order, n=n):
            to_x, to_z, to_core = owner(me, order)
            base = (to_x % 2 * 2 + to_z // 4) * 4
            c = to_z % 4 * 2 + to_core
            mine = own_at[c]
            here = own[n][base + jnp.maximum(mine, 0)]
            there = swapped[n][base + other_at[c]]
            return jnp.where(mine >= 0, here, there)

        def pack(order, rows=rows, pick=pick):
            packed[order, rows, :] = pick(order)

        def send(order, n=n, rows=rows):
            to_x, to_z, to_core = owner(me, order)
            pltpu.make_async_remote_copy(
                src_ref=packed.at[order, rows, :],
                dst_ref=received[n].at[my_slot],
                send_sem=send_sem.at[n],
                recv_sem=recv_sem.at[n],
                device_id={"dev": to_x * 16 + to_z * 2 + to_core},
                device_id_type=MESH,
            ).start()

        def step(order, carry, pack=pack, send=send):
            pack(order + 1)
            send(order)
            return carry

        pack(0)
        lax.fori_loop(0, 27, step, 0)
        pack(29)
        send(27)
        pack(30)
        send(29)
        pack(31)
        send(30)
        received[n][my_slot] = pick(28)
        send(31)

    row_mine = x * 2 + z // 4
    col_mine = z % 4 * 2 + core
    row_part = [[], []]
    col_part = [[], []]
    for c in range(2):
        for s in range(6):
            at = jnp.int32(-1)
            for i in range(32):
                x_part = jnp.where(side == c, i % 4 // 2, 1 - i % 4 // 2)
                at = jnp.where(
                    labels[c, i] == 8 * s + row_mine, x_part * 16 + i % 2 * 8, at
                )
            row_part[c].append(at)
            at = jnp.int32(-1)
            for j in range(32):
                at = jnp.where(labels[c, j] == 8 * s + col_mine, j % 8, at)
            col_part[c].append(at)

    loads[3].wait()
    for n, (first, count) in enumerate(CHUNKS):
        rows = pl.ds(first, count)
        arrived = received[n].at[pl.ds(0, OWNERS - 1)]
        pltpu.make_async_copy(arrived, arrived, recv_sem.at[n]).wait()
        for slot in range(36):
            total = front[slot, rows, :]
            for c in range(2):
                r, q = row_part[c][slot // 6], col_part[c][slot % 6]
                at = jnp.where((r >= 0) & (q >= 0), r + q, ZERO)
                total += received[n][at]
            front[slot, rows, :] = total
    for n, (first, count) in enumerate(CHUNKS):
        swaps[n].wait_send()
        sent = packed.at[pl.ds(0, OWNERS - 1), pl.ds(first, count), :]
        pltpu.make_async_copy(sent, sent, send_sem.at[n]).wait()


def body(child_tiles, l_slab, u_slab, parent_own_entries, parent_label):
    far = pl.BlockSpec(memory_space=pltpu.HBM)
    dma = pltpu.SemaphoreType.DMA
    return pl.pallas_call(
        kernel,
        name="extend_add",
        out_shape=pltpu.VMEM(parent_own_entries.shape, F32),
        in_specs=[far] * 5,
        out_specs=pl.BlockSpec(memory_space=pltpu.VMEM),
        scratch_shapes=[
            pltpu.VMEM((32, TILE, TILE), F32),
            pltpu.VMEM((8, TILE, 512), F32),
            pltpu.VMEM((512, 512), F32),
            pltpu.VMEM((512, 512), BF16),
            pltpu.VMEM((512, 512), BF16),
            pltpu.VMEM((16, TILE, TILE), F32),
            pltpu.VMEM((OWNERS, TILE, TILE), F32),
            *[pltpu.VMEM((16, count, TILE), F32) for _, count in CHUNKS],
            *[pltpu.VMEM((OWNERS + 1, count, TILE), F32) for _, count in CHUNKS],
            *[pltpu.VMEM((16, count, TILE), F32) for _, count in CHUNKS],
            pltpu.SMEM((2, 32), jnp.int32),
            pltpu.SMEM((8,), jnp.int32),
            pltpu.SMEM((8,), jnp.int32),
            pltpu.SMEM((8,), jnp.int32),
            dma((5,)),
            dma((NCH,)),
            dma((NCH,)),
            dma((NCH,)),
            dma((NCH,)),
        ],
        compiler_params=pltpu.CompilerParams(
            collective_id=0, has_side_effects=True, vmem_limit_bytes=40 * 2**20
        ),
    )(
        *[
            pltpu.with_memory_space_constraint(array, pltpu.HBM)
            for array in (
                parent_label,
                child_tiles,
                l_slab.reshape(8, TILE, 512),
                u_slab,
                parent_own_entries,
            )
        ]
    )


def solution(mesh):
    in_specs = (
        P(("sub", "dev"), None, None),
        P(("sub", "dev"), None),
        P(None, ("sub", "dev")),
        P(("sub", "dev"), None, None),
        P("sub", None),
    )
    out_specs = P(("sub", "dev"), None, None)
    return jax.shard_map(body, mesh=mesh, in_specs=in_specs, out_specs=out_specs, check_vma=False)
```

```python
import jax
import jax.numpy as jnp
from jax import lax
from jax.experimental import pallas as pl
from jax.experimental.pallas import tpu as pltpu
from jax.sharding import PartitionSpec as P

TILE = 128
F32 = jnp.float32
BF16 = jnp.bfloat16
MESH = pl.DeviceIdType.MESH
CHUNKS = ((0, 8), (8, 8), (16, 16), (32, 24), (56, 32), (88, 40))
NCH = len(CHUNKS)
FIRST = 16
EARLY = 2
OWNERS = 32
ZERO = OWNERS


def split(value):
    high = value.astype(BF16)
    return high, (value - high.astype(F32)).astype(BF16)


def kernel(labels_hbm, child_hbm, l_hbm, u_hbm, entries_hbm, front, *scratch):
    (child, child_first, left, left_first, right, right_hi, right_lo) = scratch[:7]
    outgoing_first, outgoing, packed = scratch[7:10]
    received = scratch[10 : 10 + NCH]
    own = scratch[10 + NCH : 10 + 2 * NCH]
    swapped = scratch[10 + 2 * NCH : 10 + 4 * NCH]
    labels, row_at, own_at, other_at, load_sem, swap_send, swap_recv, send_sem, recv_sem = (
        scratch[10 + 4 * NCH :]
    )
    me = lax.axis_index("dev")
    x, z, core = lax.div(me, 16), lax.rem(lax.div(me, 2), 8), lax.rem(me, 2)
    side, x_low, z_high = lax.div(x, 2), lax.rem(x, 2), lax.div(z, 4)
    partner = me + (3 - 2 * x) * 16
    my_slot = x_low * 16 + z * 2 + core
    row_class = x_low * 2 + z_high
    col_class = lax.rem(z, 4) * 2 + core

    loads = [
        pltpu.make_async_copy(source, target, load_sem.at[n])
        for n, (source, target) in enumerate(
            (
                (labels_hbm, labels),
                (u_hbm, right),
                (l_hbm.at[:, pl.ds(0, FIRST), :], left_first),
                (child_hbm.at[:, pl.ds(0, FIRST), :], child_first),
                (l_hbm, left),
                (child_hbm, child),
                (entries_hbm, front),
            )
        )
    ]
    for load in loads[:4]:
        load.start()

    flips = [(fx, fc) for fx in range(2) for fc in range(2)]
    to_core = [core, 1 - core]
    to_x_low = [x_low, 1 - x_low]
    base = [(side * 2 + to_x_low[fx]) * 16 + to_core[fc] for fx, fc in flips]

    barrier = pltpu.get_barrier_semaphore()

    def greet(device):
        pl.semaphore_signal(barrier, inc=1, device_id={"dev": device}, device_id_type=MESH)

    for step in (3, 5, 4, 2, 6, 1, 7):
        for n in range(4):
            greet(base[n] + lax.rem(z + step, 8) * 2)
        if step == 5:
            greet(partner)
    for n in (1, 2, 3):
        greet(base[n] + z * 2)
    for load in loads[4:6]:
        load.start()

    loads[0].wait()
    row_classes = [lax.rem(labels[side, row_class + 4 * k], 8) for k in range(8)]
    for c in range(8):
        at = jnp.int32(0)
        for k in range(1, 8):
            at = jnp.where(row_classes[k] == c, k, at)
        row_at[c] = at
    own_classes = [lax.rem(labels[side, col_class + 8 * m], 8) for m in range(4)]
    other_classes = [lax.rem(labels[1 - side, col_class + 8 * m], 8) for m in range(4)]
    for c in range(8):
        at = jnp.int32(-1)
        for m in range(4):
            at = jnp.where(own_classes[m] == c, m, at)
        own_at[c] = at
        at = jnp.int32(0)
        for m in range(1, 4):
            at = jnp.where(other_classes[m] == c, m, at)
        other_at[c] = at

    loads[1].wait()
    right_hi[...], right_lo[...] = split(right[...])
    loads[2].wait()
    loads[3].wait()

    def multiply(rows, columns):
        high, low = split(rows)
        hi_columns = right_hi[:, columns]
        product = jnp.dot(high, hi_columns, preferred_element_type=F32)
        product += jnp.dot(low, hi_columns, preferred_element_type=F32)
        return product + jnp.dot(high, right_lo[:, columns], preferred_element_type=F32)

    classes = [n % 2 * 2 + n // 2 for n in range(4)]
    at = [row_at[(1 - side) * 4 + c] for c in classes] + [row_at[side * 4 + c] for c in classes]
    rows = jnp.concatenate([left_first[k] for k in at], axis=0)
    for half in range(2):
        product = multiply(rows, pl.ds(half * 256, 256))
        for n, k in enumerate(at):
            for part in range(2):
                m = 2 * half + part
                tile = product[n * FIRST : (n + 1) * FIRST, part * TILE : (part + 1) * TILE]
                tile = child_first[k * 4 + m] - tile
                if n < 4:
                    outgoing_first[n * 4 + m] = tile
                else:
                    for first, count in CHUNKS[:EARLY]:
                        own[0 if first == 0 else 1][(n - 4) * 4 + m] = tile[first : first + count]
    pl.semaphore_wait(barrier, OWNERS)

    swaps = []
    for n, (first, count) in enumerate(CHUNKS):
        source = outgoing_first if n < EARLY else outgoing
        for half in range(2):
            tiles = pl.ds(half * 8, 8)
            swaps.append(
                pltpu.make_async_remote_copy(
                    src_ref=source.at[tiles, pl.ds(first, count), :],
                    dst_ref=swapped[2 * n + half],
                    send_sem=swap_send.at[2 * n + half],
                    recv_sem=swap_recv.at[2 * n + half],
                    device_id={"dev": partner},
                    device_id_type=MESH,
                )
            )
    for swap in swaps[: 2 * EARLY]:
        swap.start()

    loads[4].wait()
    loads[5].wait()

    def update(c, put):
        ks = [row_at[c], row_at[c + 2]]
        rows = jnp.concatenate([left[k] for k in ks], axis=0)
        for half in range(2):
            product = multiply(rows, pl.ds(half * 256, 256))
            for n, k in enumerate(ks):
                for part in range(2):
                    m = 2 * half + part
                    tile = product[n * TILE : (n + 1) * TILE, part * TILE : (part + 1) * TILE]
                    put(n, m, child[k * 4 + m] - tile)

    def other_step(pair, carry):
        def put(n, m, tile):
            outgoing[(pair * 2 + n) * 4 + m] = tile

        update((1 - side) * 4 + pair, put)
        return carry

    def own_step(pair, carry):
        def put(n, m, tile):
            for part, (first, count) in list(zip(own, CHUNKS))[EARLY:]:
                part[(pair * 2 + n) * 4 + m] = tile[first : first + count]

        update(side * 4 + pair, put)
        return carry

    lax.fori_loop(0, 2, other_step, 0)
    for swap in swaps[2 * EARLY :]:
        swap.start()
    loads[6].start()
    for n, (first, count) in enumerate(CHUNKS):
        rows = pl.ds(first, count)
        received[n][ZERO] = jnp.zeros((count, TILE), F32)
        if n == 1:
            lax.fori_loop(0, 2, own_step, 0)

        def send(to_z, n=n, rows=rows):
            for i in range(4):

                def start(i=i):
                    pltpu.make_async_remote_copy(
                        src_ref=packed.at[to_z * 4 + i, rows, :],
                        dst_ref=received[n].at[my_slot],
                        send_sem=send_sem.at[n],
                        recv_sem=recv_sem.at[n],
                        device_id={"dev": base[i] + to_z * 2},
                        device_id_type=MESH,
                    ).start()

                if i:
                    start()
                else:
                    pl.when(to_z != z)(start)

        for half in range(2):
            first_z, way = (0, 1) if half == 0 else (7, -1)

            def pick(to_z, fx, fc, n=n, half=half):
                c = lax.rem(to_z, 4) * 2 + to_core[fc]
                mine, other = own_at[c], other_at[c]
                place = to_x_low[fx] * 4
                here = own[n][half * 8 + place + jnp.maximum(mine, 0)]
                there = swapped[2 * n + half][place + other]
                return jnp.where(mine >= 0, here, there)

            def pack(to_z, rows=rows, pick=pick):
                for i, (fx, fc) in enumerate(flips):
                    packed[to_z * 4 + i, rows, :] = pick(to_z, fx, fc)

            def step(q, carry, pack=pack, send=send, first_z=first_z, way=way):
                pack(first_z + way * (q + 1))
                send(first_z + way * q)
                return carry

            swaps[2 * n + half].wait_recv()
            pack(jnp.int32(first_z))
            lax.fori_loop(0, 3, step, 0)

            def keep(n=n, pick=pick):
                received[n][my_slot] = pick(z, 0, 0)

            pl.when(z_high == half)(keep)
            send(jnp.int32(first_z + 3 * way))

    row_part = [[], []]
    col_part = [[], []]
    for c in range(2):
        for s in range(6):
            at = jnp.int32(-1)
            for i in range(32):
                x_part = jnp.where(side == c, i % 4 // 2, 1 - i % 4 // 2)
                here = labels[c, i] == 8 * s + x * 2 + z_high
                at = jnp.where(here, x_part * 16 + i % 2 * 8, at)
            row_part[c].append(at)
            at = jnp.int32(-1)
            for j in range(32):
                at = jnp.where(labels[c, j] == 8 * s + col_class, j % 8, at)
            col_part[c].append(at)

    loads[6].wait()
    for n, (first, count) in enumerate(CHUNKS):
        rows = pl.ds(first, count)
        arrived = received[n].at[pl.ds(0, OWNERS - 1)]
        pltpu.make_async_copy(arrived, arrived, recv_sem.at[n]).wait()
        for slot in range(36):
            total = front[slot, rows, :]
            for c in range(2):
                r, q = row_part[c][slot // 6], col_part[c][slot % 6]
                total += received[n][jnp.where((r >= 0) & (q >= 0), r + q, ZERO)]
            front[slot, rows, :] = total
    for swap in swaps:
        swap.wait_send()
    for n, (first, count) in enumerate(CHUNKS):
        sent = packed.at[pl.ds(0, OWNERS - 1), pl.ds(first, count), :]
        pltpu.make_async_copy(sent, sent, send_sem.at[n]).wait()


def body(child_tiles, l_slab, u_slab, parent_own_entries, parent_label):
    far = pl.BlockSpec(memory_space=pltpu.HBM)
    dma = pltpu.SemaphoreType.DMA
    return pl.pallas_call(
        kernel,
        name="extend_add",
        out_shape=pltpu.VMEM(parent_own_entries.shape, F32),
        in_specs=[far] * 5,
        out_specs=pl.BlockSpec(memory_space=pltpu.VMEM),
        scratch_shapes=[
            pltpu.VMEM((32, TILE, TILE), F32),
            pltpu.VMEM((32, FIRST, TILE), F32),
            pltpu.VMEM((8, TILE, 512), F32),
            pltpu.VMEM((8, FIRST, 512), F32),
            pltpu.VMEM((512, 512), F32),
            pltpu.VMEM((512, 512), BF16),
            pltpu.VMEM((512, 512), BF16),
            pltpu.VMEM((16, FIRST, TILE), F32),
            pltpu.VMEM((16, TILE, TILE), F32),
            pltpu.VMEM((OWNERS, TILE, TILE), F32),
            *[pltpu.VMEM((OWNERS + 1, count, TILE), F32) for _, count in CHUNKS],
            *[pltpu.VMEM((16, count, TILE), F32) for _, count in CHUNKS],
            *[pltpu.VMEM((8, count, TILE), F32) for _, count in CHUNKS for _ in range(2)],
            pltpu.SMEM((2, 32), jnp.int32),
            pltpu.SMEM((8,), jnp.int32),
            pltpu.SMEM((8,), jnp.int32),
            pltpu.SMEM((8,), jnp.int32),
            dma((7,)),
            dma((2 * NCH,)),
            dma((2 * NCH,)),
            dma((NCH,)),
            dma((NCH,)),
        ],
        compiler_params=pltpu.CompilerParams(
            collective_id=0, has_side_effects=True, vmem_limit_bytes=40 * 2**20
        ),
    )(
        *[
            pltpu.with_memory_space_constraint(array, pltpu.HBM)
            for array in (
                parent_label,
                child_tiles,
                l_slab.reshape(8, TILE, 512),
                u_slab,
                parent_own_entries,
            )
        ]
    )


def solution(mesh):
    in_specs = (
        P(("sub", "dev"), None, None),
        P(("sub", "dev"), None),
        P(None, ("sub", "dev")),
        P(("sub", "dev"), None, None),
        P("sub", None),
    )
    out_specs = P(("sub", "dev"), None, None)
    return jax.shard_map(body, mesh=mesh, in_specs=in_specs, out_specs=out_specs, check_vma=False)
```

```python
import jax
import jax.numpy as jnp
from jax import lax
from jax.experimental import pallas as pl
from jax.experimental.pallas import tpu as pltpu
from jax.sharding import PartitionSpec as P

TILE = 128
F32 = jnp.float32
BF16 = jnp.bfloat16
MESH = pl.DeviceIdType.MESH
CHUNKS = ((0, 8), (8, 8), (16, 24), (40, 40), (80, 48))
NCH = len(CHUNKS)
FIRST = 16
EARLY = 2
APART = 1
ORDERS = (((0, 1, 2, 3), (7, 6, 5, 4)),) * NCH
OWNERS = 32
ZERO = OWNERS


def split(value):
    high = value.astype(BF16)
    return high, (value - high.astype(F32)).astype(BF16)


def kernel(labels_hbm, child_hbm, l_hbm, u_hbm, entries_hbm, front, *scratch):
    (child, child_first, left, left_first, right, right_hi, right_lo) = scratch[:7]
    outgoing_first, outgoing, packed = scratch[7:10]
    received = scratch[10 : 10 + NCH]
    own = scratch[10 + NCH : 10 + 2 * NCH]
    swapped = scratch[10 + 2 * NCH : 10 + 6 * NCH]
    labels, row_at, own_at, other_at, load_sem, known_sem = scratch[10 + 6 * NCH :][:6]
    swap_send, swap_recv, send_sem, recv_sem = scratch[10 + 6 * NCH :][6:]
    me = lax.axis_index("dev")
    x, z, core = lax.div(me, 16), lax.rem(lax.div(me, 2), 8), lax.rem(me, 2)
    side, x_low, z_high = lax.div(x, 2), lax.rem(x, 2), lax.div(z, 4)
    partner = me + (3 - 2 * x) * 16
    my_slot = x_low * 16 + z * 2 + core
    row_class = x_low * 2 + z_high
    col_class = lax.rem(z, 4) * 2 + core

    loads = [
        pltpu.make_async_copy(source, target, load_sem.at[n])
        for n, (source, target) in enumerate(
            (
                (labels_hbm, labels),
                (u_hbm, right),
                (l_hbm.at[:, pl.ds(0, FIRST), :], left_first),
                (child_hbm.at[:, pl.ds(0, FIRST), :], child_first),
                (l_hbm, left),
                (child_hbm, child),
                (entries_hbm, front),
            )
        )
    ]
    for load in loads[:4]:
        load.start()

    to_core = [core, 1 - core]
    base = [[(side * 2 + xl) * 16 + to_core[fc] for fc in range(2)] for xl in range(2)]

    barrier = pltpu.get_barrier_semaphore()

    def signal(semaphore, device):
        pl.semaphore_signal(semaphore, inc=1, device_id={"dev": device}, device_id_type=MESH)

    def along(step):
        return lax.rem(z + step + 8, 8) * 2

    mine = (side * 2 + x_low) * 16 + core
    others = [
        (side * 2 + x_low) * 16 + 1 - core,
        (side * 2 + 1 - x_low) * 16 + core,
        (side * 2 + 1 - x_low) * 16 + 1 - core,
    ]
    for step in (1, -1):
        for column in others[::-1] + [mine]:
            signal(barrier, column + along(step))
    signal(barrier, partner)
    for column in others:
        signal(barrier, column + z * 2)
    for load in loads[4:6]:
        load.start()

    loads[0].wait()
    row_classes = [lax.rem(labels[side, row_class + 4 * k], 8) for k in range(8)]
    for c in range(8):
        at = jnp.int32(0)
        for k in range(1, 8):
            at = jnp.where(row_classes[k] == c, k, at)
        row_at[c] = at
    own_classes = [lax.rem(labels[side, col_class + 8 * m], 8) for m in range(4)]
    other_classes = [lax.rem(labels[1 - side, col_class + 8 * m], 8) for m in range(4)]
    for c in range(8):
        at = jnp.int32(-1)
        for m in range(4):
            at = jnp.where(own_classes[m] == c, m, at)
        own_at[c] = at
        at = jnp.int32(0)
        for m in range(1, 4):
            at = jnp.where(other_classes[m] == c, m, at)
        other_at[c] = at

    loads[1].wait()
    right_hi[...], right_lo[...] = split(right[...])
    loads[2].wait()
    loads[3].wait()

    def multiply(rows, columns):
        high, low = split(rows)
        hi_columns = right_hi[:, columns]
        product = jnp.dot(high, hi_columns, preferred_element_type=F32)
        product += jnp.dot(low, hi_columns, preferred_element_type=F32)
        return product + jnp.dot(high, right_lo[:, columns], preferred_element_type=F32)

    classes = [n % 2 * 2 + n // 2 for n in range(4)]
    at = [row_at[(1 - side) * 4 + c] for c in classes] + [row_at[side * 4 + c] for c in classes]
    rows = jnp.concatenate([left_first[k] for k in at], axis=0)
    for half in range(2):
        product = multiply(rows, pl.ds(half * 256, 256))
        for n, k in enumerate(at):
            for part in range(2):
                m = 2 * half + part
                tile = product[n * FIRST : (n + 1) * FIRST, part * TILE : (part + 1) * TILE]
                tile = child_first[k * 4 + m] - tile
                if n < 4:
                    outgoing_first[n * 4 + m] = tile
                else:
                    for first, count in CHUNKS[:EARLY]:
                        own[0 if first == 0 else 1][(n - 4) * 4 + m] = tile[first : first + count]
    pl.semaphore_wait(barrier, 12)

    swaps = []
    for n, (first, count) in enumerate(CHUNKS):
        source = outgoing_first if n < EARLY else outgoing
        for piece in range(4):
            tiles = pl.ds(piece * 4, 4)
            swaps.append(
                pltpu.make_async_remote_copy(
                    src_ref=source.at[tiles, pl.ds(first, count), :],
                    dst_ref=swapped[4 * n + piece],
                    send_sem=swap_send.at[4 * n + piece],
                    recv_sem=swap_recv.at[4 * n + piece],
                    device_id={"dev": partner},
                    device_id_type=MESH,
                )
            )
    for swap in swaps[: 4 * EARLY]:
        swap.start()
    for step in (1, -1):
        signal(known_sem.at[0], mine + along(step))

    loads[4].wait()
    loads[5].wait()
    pl.semaphore_wait(known_sem.at[0], 2)
    for step in (2, -2):
        signal(known_sem.at[1], mine + along(step))

    def update(c, put):
        ks = [row_at[c], row_at[c + 2]]
        rows = jnp.concatenate([left[k] for k in ks], axis=0)
        for half in range(2):
            product = multiply(rows, pl.ds(half * 256, 256))
            for n, k in enumerate(ks):
                for part in range(2):
                    m = 2 * half + part
                    tile = product[n * TILE : (n + 1) * TILE, part * TILE : (part + 1) * TILE]
                    put(n, m, child[k * 4 + m] - tile)

    def other_step(pair, carry):
        def put(n, m, tile):
            outgoing[(pair * 2 + n) * 4 + m] = tile

        update((1 - side) * 4 + pair, put)
        return carry

    def own_step(pair, carry):
        def put(n, m, tile):
            for part, (first, count) in list(zip(own, CHUNKS))[EARLY:]:
                part[(pair * 2 + n) * 4 + m] = tile[first : first + count]

        update(side * 4 + pair, put)
        return carry

    lax.fori_loop(0, 2, other_step, 0)
    for swap in swaps[4 * EARLY :]:
        swap.start()
    loads[6].start()
    pl.semaphore_wait(known_sem.at[1], 2)

    for n, (first, count) in enumerate(CHUNKS):
        rows = pl.ds(first, count)
        received[n][ZERO] = jnp.zeros((count, TILE), F32)
        if n == 1:
            lax.fori_loop(0, 2, own_step, 0)

        for pieces in ((0,), (1,), (2,), (3,)) if n < APART else ((0, 1), (2, 3)):
            half = pieces[0] // 2
            order = ORDERS[n][half]

            def pick(to_z, fc, piece, n=n):
                c = lax.rem(to_z, 4) * 2 + to_core[fc]
                mine, other = own_at[c], other_at[c]
                here = own[n][piece * 4 + jnp.maximum(mine, 0)]
                there = swapped[4 * n + piece][other]
                return jnp.where(mine >= 0, here, there)

            def pack(to_z, rows=rows, pick=pick, pieces=pieces):
                for piece in pieces:
                    for fc in range(2):
                        packed[to_z * 4 + piece % 2 * 2 + fc, rows, :] = pick(to_z, fc, piece)

            def send(to_z, n=n, rows=rows, pieces=pieces):
                for piece in pieces:
                    xl = piece % 2
                    for fc in range(2):

                        def start(fc=fc, xl=xl):
                            pltpu.make_async_remote_copy(
                                src_ref=packed.at[to_z * 4 + xl * 2 + fc, rows, :],
                                dst_ref=received[n].at[my_slot],
                                send_sem=send_sem.at[n],
                                recv_sem=recv_sem.at[n],
                                device_id={"dev": base[xl][fc] + to_z * 2},
                                device_id_type=MESH,
                            ).start()

                        if fc:
                            start()
                        else:
                            pl.when((to_z != z) | (x_low != xl))(start)

            for piece in pieces:
                swaps[4 * n + piece].wait_recv()
            pack(order[0])
            for to_z, next_z in zip(order, order[1:]):
                pack(next_z)
                send(to_z)
            for piece in pieces:

                def keep(n=n, pick=pick, piece=piece):
                    received[n][my_slot] = pick(z, 0, piece)

                pl.when((z_high == half) & (x_low == piece % 2))(keep)
            send(order[-1])

    row_part = [[], []]
    col_part = [[], []]
    for c in range(2):
        for s in range(6):
            at = jnp.int32(-1)
            for i in range(32):
                x_part = jnp.where(side == c, i % 4 // 2, 1 - i % 4 // 2)
                here = labels[c, i] == 8 * s + x * 2 + z_high
                at = jnp.where(here, x_part * 16 + i % 2 * 8, at)
            row_part[c].append(at)
            at = jnp.int32(-1)
            for j in range(32):
                at = jnp.where(labels[c, j] == 8 * s + col_class, j % 8, at)
            col_part[c].append(at)

    loads[6].wait()
    for n, (first, count) in enumerate(CHUNKS):
        rows = pl.ds(first, count)
        arrived = received[n].at[pl.ds(0, OWNERS - 1)]
        pltpu.make_async_copy(arrived, arrived, recv_sem.at[n]).wait()
        for slot in range(36):
            total = front[slot, rows, :]
            for c in range(2):
                r, q = row_part[c][slot // 6], col_part[c][slot % 6]
                total += received[n][jnp.where((r >= 0) & (q >= 0), r + q, ZERO)]
            front[slot, rows, :] = total
    for swap in swaps:
        swap.wait_send()
    for n, (first, count) in enumerate(CHUNKS):
        sent = packed.at[pl.ds(0, OWNERS - 1), pl.ds(first, count), :]
        pltpu.make_async_copy(sent, sent, send_sem.at[n]).wait()


def body(child_tiles, l_slab, u_slab, parent_own_entries, parent_label):
    far = pl.BlockSpec(memory_space=pltpu.HBM)
    dma = pltpu.SemaphoreType.DMA
    return pl.pallas_call(
        kernel,
        name="extend_add",
        out_shape=pltpu.VMEM(parent_own_entries.shape, F32),
        in_specs=[far] * 5,
        out_specs=pl.BlockSpec(memory_space=pltpu.VMEM),
        scratch_shapes=[
            pltpu.VMEM((32, TILE, TILE), F32),
            pltpu.VMEM((32, FIRST, TILE), F32),
            pltpu.VMEM((8, TILE, 512), F32),
            pltpu.VMEM((8, FIRST, 512), F32),
            pltpu.VMEM((512, 512), F32),
            pltpu.VMEM((512, 512), BF16),
            pltpu.VMEM((512, 512), BF16),
            pltpu.VMEM((16, FIRST, TILE), F32),
            pltpu.VMEM((16, TILE, TILE), F32),
            pltpu.VMEM((OWNERS, TILE, TILE), F32),
            *[pltpu.VMEM((OWNERS + 1, count, TILE), F32) for _, count in CHUNKS],
            *[pltpu.VMEM((16, count, TILE), F32) for _, count in CHUNKS],
            *[pltpu.VMEM((4, count, TILE), F32) for _, count in CHUNKS for _ in range(4)],
            pltpu.SMEM((2, 32), jnp.int32),
            pltpu.SMEM((8,), jnp.int32),
            pltpu.SMEM((8,), jnp.int32),
            pltpu.SMEM((8,), jnp.int32),
            dma((7,)),
            pltpu.SemaphoreType.REGULAR((2,)),
            dma((4 * NCH,)),
            dma((4 * NCH,)),
            dma((NCH,)),
            dma((NCH,)),
        ],
        compiler_params=pltpu.CompilerParams(
            collective_id=0, has_side_effects=True, vmem_limit_bytes=40 * 2**20
        ),
    )(
        *[
            pltpu.with_memory_space_constraint(array, pltpu.HBM)
            for array in (
                parent_label,
                child_tiles,
                l_slab.reshape(8, TILE, 512),
                u_slab,
                parent_own_entries,
            )
        ]
    )


def solution(mesh):
    in_specs = (
        P(("sub", "dev"), None, None),
        P(("sub", "dev"), None),
        P(None, ("sub", "dev")),
        P(("sub", "dev"), None, None),
        P("sub", None),
    )
    out_specs = P(("sub", "dev"), None, None)
    return jax.shard_map(body, mesh=mesh, in_specs=in_specs, out_specs=out_specs, check_vma=False)
```

```python
import jax
import jax.numpy as jnp
from jax import lax
from jax.experimental import pallas as pl
from jax.experimental.pallas import tpu as pltpu
from jax.sharding import PartitionSpec as P

TILE = 128
F32 = jnp.float32
BF16 = jnp.bfloat16
MESH = pl.DeviceIdType.MESH
CHUNKS = ((0, 8), (8, 8), (16, 16), (32, 40), (72, 56))
NCH = len(CHUNKS)
FIRST = 16
EARLY = 2
APART = 1
RELAY, FROM, VIA, TO = 2, 6, 3, 2
ORDERS = (((0, 1, 2, 3), (7, 6, 5, 4)),) * NCH
OWNERS = 32
ZERO = OWNERS


def split(value):
    high = value.astype(BF16)
    return high, (value - high.astype(F32)).astype(BF16)


def kernel(labels_hbm, child_hbm, l_hbm, u_hbm, entries_hbm, front, *scratch):
    passing, pass_sem = scratch[-2:]
    scratch = scratch[:-2]
    (child, child_first, left, left_first, right, right_hi, right_lo) = scratch[:7]
    outgoing_first, outgoing, packed = scratch[7:10]
    received = scratch[10 : 10 + NCH]
    own = scratch[10 + NCH : 10 + 2 * NCH]
    swapped = scratch[10 + 2 * NCH : 10 + 6 * NCH]
    labels, row_at, own_at, other_at, load_sem, known_sem = scratch[10 + 6 * NCH :][:6]
    swap_send, swap_recv, send_sem, recv_sem = scratch[10 + 6 * NCH :][6:]
    me = lax.axis_index("dev")
    x, z, core = lax.div(me, 16), lax.rem(lax.div(me, 2), 8), lax.rem(me, 2)
    side, x_low, z_high = lax.div(x, 2), lax.rem(x, 2), lax.div(z, 4)
    partner = me + (3 - 2 * x) * 16
    my_slot = x_low * 16 + z * 2 + core
    row_class = x_low * 2 + z_high
    col_class = lax.rem(z, 4) * 2 + core

    loads = [
        pltpu.make_async_copy(source, target, load_sem.at[n])
        for n, (source, target) in enumerate(
            (
                (labels_hbm, labels),
                (u_hbm, right),
                (l_hbm.at[:, pl.ds(0, FIRST), :], left_first),
                (child_hbm.at[:, pl.ds(0, FIRST), :], child_first),
                (l_hbm, left),
                (child_hbm, child),
                (entries_hbm, front),
            )
        )
    ]
    for load in loads[:4]:
        load.start()

    to_core = [core, 1 - core]
    base = [[(side * 2 + xl) * 16 + to_core[fc] for fc in range(2)] for xl in range(2)]

    barrier = pltpu.get_barrier_semaphore()

    def signal(semaphore, device):
        pl.semaphore_signal(semaphore, inc=1, device_id={"dev": device}, device_id_type=MESH)

    def along(step):
        return lax.rem(z + step + 8, 8) * 2

    mine = (side * 2 + x_low) * 16 + core
    others = [
        (side * 2 + x_low) * 16 + 1 - core,
        (side * 2 + 1 - x_low) * 16 + core,
        (side * 2 + 1 - x_low) * 16 + 1 - core,
    ]
    for step in (1, -1):
        for column in others[::-1] + [mine]:
            signal(barrier, column + along(step))
    signal(barrier, partner)
    for column in others:
        signal(barrier, column + z * 2)
    for load in loads[4:6]:
        load.start()

    loads[0].wait()
    row_classes = [lax.rem(labels[side, row_class + 4 * k], 8) for k in range(8)]
    for c in range(8):
        at = jnp.int32(0)
        for k in range(1, 8):
            at = jnp.where(row_classes[k] == c, k, at)
        row_at[c] = at
    own_classes = [lax.rem(labels[side, col_class + 8 * m], 8) for m in range(4)]
    other_classes = [lax.rem(labels[1 - side, col_class + 8 * m], 8) for m in range(4)]
    for c in range(8):
        at = jnp.int32(-1)
        for m in range(4):
            at = jnp.where(own_classes[m] == c, m, at)
        own_at[c] = at
        at = jnp.int32(0)
        for m in range(1, 4):
            at = jnp.where(other_classes[m] == c, m, at)
        other_at[c] = at

    loads[1].wait()
    right_hi[...], right_lo[...] = split(right[...])
    loads[2].wait()
    loads[3].wait()

    def multiply(rows, columns):
        high, low = split(rows)
        hi_columns = right_hi[:, columns]
        product = jnp.dot(high, hi_columns, preferred_element_type=F32)
        product += jnp.dot(low, hi_columns, preferred_element_type=F32)
        return product + jnp.dot(high, right_lo[:, columns], preferred_element_type=F32)

    classes = [n % 2 * 2 + n // 2 for n in range(4)]
    at = [row_at[(1 - side) * 4 + c] for c in classes] + [row_at[side * 4 + c] for c in classes]
    rows = jnp.concatenate([left_first[k] for k in at], axis=0)
    for half in range(2):
        product = multiply(rows, pl.ds(half * 256, 256))
        for n, k in enumerate(at):
            for part in range(2):
                m = 2 * half + part
                tile = product[n * FIRST : (n + 1) * FIRST, part * TILE : (part + 1) * TILE]
                tile = child_first[k * 4 + m] - tile
                if n < 4:
                    outgoing_first[n * 4 + m] = tile
                else:
                    for first, count in CHUNKS[:EARLY]:
                        own[0 if first == 0 else 1][(n - 4) * 4 + m] = tile[first : first + count]
    pl.semaphore_wait(barrier, 12)

    swaps = []
    for n, (first, count) in enumerate(CHUNKS):
        source = outgoing_first if n < EARLY else outgoing
        for piece in range(4):
            tiles = pl.ds(piece * 4, 4)
            swaps.append(
                pltpu.make_async_remote_copy(
                    src_ref=source.at[tiles, pl.ds(first, count), :],
                    dst_ref=swapped[4 * n + piece],
                    send_sem=swap_send.at[4 * n + piece],
                    recv_sem=swap_recv.at[4 * n + piece],
                    device_id={"dev": partner},
                    device_id_type=MESH,
                )
            )
    for swap in swaps[: 4 * EARLY]:
        swap.start()
    for step in (1, -1):
        signal(known_sem.at[0], mine + along(step))

    loads[4].wait()
    loads[5].wait()
    pl.semaphore_wait(known_sem.at[0], 2)
    for step in (2, -2):
        signal(known_sem.at[1], mine + along(step))

    def update(c, put):
        ks = [row_at[c], row_at[c + 2]]
        rows = jnp.concatenate([left[k] for k in ks], axis=0)
        for half in range(2):
            product = multiply(rows, pl.ds(half * 256, 256))
            for n, k in enumerate(ks):
                for part in range(2):
                    m = 2 * half + part
                    tile = product[n * TILE : (n + 1) * TILE, part * TILE : (part + 1) * TILE]
                    put(n, m, child[k * 4 + m] - tile)

    def other_step(pair, carry):
        def put(n, m, tile):
            outgoing[(pair * 2 + n) * 4 + m] = tile

        update((1 - side) * 4 + pair, put)
        return carry

    def own_step(pair, carry):
        def put(n, m, tile):
            for part, (first, count) in list(zip(own, CHUNKS))[EARLY:]:
                part[(pair * 2 + n) * 4 + m] = tile[first : first + count]

        update(side * 4 + pair, put)
        return carry

    lax.fori_loop(0, 2, other_step, 0)
    for swap in swaps[4 * EARLY :]:
        swap.start()
    loads[6].start()
    pl.semaphore_wait(known_sem.at[1], 2)

    for n, (first, count) in enumerate(CHUNKS):
        rows = pl.ds(first, count)
        received[n][ZERO] = jnp.zeros((count, TILE), F32)
        if n == 1:
            lax.fori_loop(0, 2, own_step, 0)

        for pieces in ((0,), (1,), (2,), (3,)) if n < APART else ((0, 1), (2, 3)):
            half = pieces[0] // 2
            order = ORDERS[n][half]

            def pick(to_z, fc, piece, n=n):
                c = lax.rem(to_z, 4) * 2 + to_core[fc]
                mine, other = own_at[c], other_at[c]
                here = own[n][piece * 4 + jnp.maximum(mine, 0)]
                there = swapped[4 * n + piece][other]
                return jnp.where(mine >= 0, here, there)

            def pack(to_z, rows=rows, pick=pick, pieces=pieces):
                for piece in pieces:
                    for fc in range(2):
                        packed[to_z * 4 + piece % 2 * 2 + fc, rows, :] = pick(to_z, fc, piece)

            def send_direct(to_z, n=n, rows=rows, pieces=pieces):
                for piece in pieces:
                    xl = piece % 2
                    for fc in range(2):

                        def start(fc=fc, xl=xl):
                            pltpu.make_async_remote_copy(
                                src_ref=packed.at[to_z * 4 + xl * 2 + fc, rows, :],
                                dst_ref=received[n].at[my_slot],
                                send_sem=send_sem.at[n],
                                recv_sem=recv_sem.at[n],
                                device_id={"dev": base[xl][fc] + to_z * 2},
                                device_id_type=MESH,
                            ).start()

                        if fc:
                            start()
                        else:
                            pl.when((to_z != z) | (x_low != xl))(start)

            def send_indirect(rows=rows, n=n):
                pltpu.make_async_remote_copy(
                    src_ref=packed.at[pl.ds(TO * 4, 4), rows, :],
                    dst_ref=passing,
                    send_sem=send_sem.at[n],
                    recv_sem=pass_sem.at[0],
                    device_id={"dev": mine + VIA * 2},
                    device_id_type=MESH,
                ).start()

            def send(to_z, n=n, direct=send_direct, indirect=send_indirect):
                if n == RELAY and to_z == TO:
                    pl.when(z == FROM)(indirect)
                    pl.when(z != FROM)(lambda: direct(to_z))
                else:
                    direct(to_z)

            for piece in pieces:
                swaps[4 * n + piece].wait_recv()
            pack(order[0])
            for to_z, next_z in zip(order, order[1:]):
                pack(next_z)
                send(to_z)
            for piece in pieces:

                def keep(n=n, pick=pick, piece=piece):
                    received[n][my_slot] = pick(z, 0, piece)

                pl.when((z_high == half) & (x_low == piece % 2))(keep)
            send(order[-1])

        if n == RELAY + 1:

            def forward():
                pltpu.make_async_copy(passing, passing, pass_sem.at[0]).wait()
                for xl in range(2):
                    for fc in range(2):
                        pltpu.make_async_remote_copy(
                            src_ref=passing.at[xl * 2 + fc],
                            dst_ref=received[RELAY].at[x_low * 16 + FROM * 2 + core],
                            send_sem=pass_sem.at[1],
                            recv_sem=recv_sem.at[RELAY],
                            device_id={"dev": base[xl][fc] + TO * 2},
                            device_id_type=MESH,
                        ).start()

            pl.when(z == VIA)(forward)

    row_part = [[], []]
    col_part = [[], []]
    for c in range(2):
        for s in range(6):
            at = jnp.int32(-1)
            for i in range(32):
                x_part = jnp.where(side == c, i % 4 // 2, 1 - i % 4 // 2)
                here = labels[c, i] == 8 * s + x * 2 + z_high
                at = jnp.where(here, x_part * 16 + i % 2 * 8, at)
            row_part[c].append(at)
            at = jnp.int32(-1)
            for j in range(32):
                at = jnp.where(labels[c, j] == 8 * s + col_class, j % 8, at)
            col_part[c].append(at)

    loads[6].wait()
    for n, (first, count) in enumerate(CHUNKS):
        rows = pl.ds(first, count)
        arrived = received[n].at[pl.ds(0, OWNERS - 1)]
        pltpu.make_async_copy(arrived, arrived, recv_sem.at[n]).wait()
        for slot in range(36):
            total = front[slot, rows, :]
            for c in range(2):
                r, q = row_part[c][slot // 6], col_part[c][slot % 6]
                total += received[n][jnp.where((r >= 0) & (q >= 0), r + q, ZERO)]
            front[slot, rows, :] = total
    pl.when(z == VIA)(lambda: pltpu.make_async_copy(passing, passing, pass_sem.at[1]).wait())
    for swap in swaps:
        swap.wait_send()
    for n, (first, count) in enumerate(CHUNKS):
        sent = packed.at[pl.ds(0, OWNERS - 1), pl.ds(first, count), :]
        pltpu.make_async_copy(sent, sent, send_sem.at[n]).wait()


def body(child_tiles, l_slab, u_slab, parent_own_entries, parent_label):
    far = pl.BlockSpec(memory_space=pltpu.HBM)
    dma = pltpu.SemaphoreType.DMA
    return pl.pallas_call(
        kernel,
        name="extend_add",
        out_shape=pltpu.VMEM(parent_own_entries.shape, F32),
        in_specs=[far] * 5,
        out_specs=pl.BlockSpec(memory_space=pltpu.VMEM),
        scratch_shapes=[
            pltpu.VMEM((32, TILE, TILE), F32),
            pltpu.VMEM((32, FIRST, TILE), F32),
            pltpu.VMEM((8, TILE, 512), F32),
            pltpu.VMEM((8, FIRST, 512), F32),
            pltpu.VMEM((512, 512), F32),
            pltpu.VMEM((512, 512), BF16),
            pltpu.VMEM((512, 512), BF16),
            pltpu.VMEM((16, FIRST, TILE), F32),
            pltpu.VMEM((16, TILE, TILE), F32),
            pltpu.VMEM((OWNERS, TILE, TILE), F32),
            *[pltpu.VMEM((OWNERS + 1, count, TILE), F32) for _, count in CHUNKS],
            *[pltpu.VMEM((16, count, TILE), F32) for _, count in CHUNKS],
            *[pltpu.VMEM((4, count, TILE), F32) for _, count in CHUNKS for _ in range(4)],
            pltpu.SMEM((2, 32), jnp.int32),
            pltpu.SMEM((8,), jnp.int32),
            pltpu.SMEM((8,), jnp.int32),
            pltpu.SMEM((8,), jnp.int32),
            dma((7,)),
            pltpu.SemaphoreType.REGULAR((2,)),
            dma((4 * NCH,)),
            dma((4 * NCH,)),
            dma((NCH,)),
            dma((NCH,)),
            pltpu.VMEM((4, CHUNKS[RELAY][1], TILE), F32),
            dma((2,)),
        ],
        compiler_params=pltpu.CompilerParams(
            collective_id=0, has_side_effects=True, vmem_limit_bytes=40 * 2**20
        ),
    )(
        *[
            pltpu.with_memory_space_constraint(array, pltpu.HBM)
            for array in (
                parent_label,
                child_tiles,
                l_slab.reshape(8, TILE, 512),
                u_slab,
                parent_own_entries,
            )
        ]
    )


def solution(mesh):
    in_specs = (
        P(("sub", "dev"), None, None),
        P(("sub", "dev"), None),
        P(None, ("sub", "dev")),
        P(("sub", "dev"), None, None),
        P("sub", None),
    )
    out_specs = P(("sub", "dev"), None, None)
    return jax.shard_map(body, mesh=mesh, in_specs=in_specs, out_specs=out_specs, check_vma=False)
```

```python
import jax
import jax.numpy as jnp
from jax import lax
from jax.experimental import pallas as pl
from jax.experimental.pallas import tpu as pltpu
from jax.sharding import PartitionSpec as P

TILE = 128
F32 = jnp.float32
BF16 = jnp.bfloat16
MESH = pl.DeviceIdType.MESH
CHUNKS = ((0, 8), (8, 8), (16, 16), (32, 40), (72, 56))
NCH = len(CHUNKS)
FIRST = 16
EARLY = 2
APART = 1
RELAY = 2
DETOURS = ((6, 3, 2), (3, 6, 7))
ORDERS = (((0, 1, 2, 3), (7, 6, 5, 4)),) * NCH
OWNERS = 32
ZERO = OWNERS


def split(value):
    high = value.astype(BF16)
    return high, (value - high.astype(F32)).astype(BF16)


def kernel(labels_hbm, child_hbm, l_hbm, u_hbm, entries_hbm, front, *scratch):
    passing, pass_sem = scratch[-2:]
    scratch = scratch[:-2]
    (child, child_first, left, left_first, right, right_hi, right_lo) = scratch[:7]
    outgoing_first, outgoing, packed = scratch[7:10]
    received = scratch[10 : 10 + NCH]
    own = scratch[10 + NCH : 10 + 2 * NCH]
    swapped = scratch[10 + 2 * NCH : 10 + 6 * NCH]
    labels, row_at, own_at, other_at, load_sem, known_sem = scratch[10 + 6 * NCH :][:6]
    swap_send, swap_recv, send_sem, recv_sem = scratch[10 + 6 * NCH :][6:]
    me = lax.axis_index("dev")
    x, z, core = lax.div(me, 16), lax.rem(lax.div(me, 2), 8), lax.rem(me, 2)
    side, x_low, z_high = lax.div(x, 2), lax.rem(x, 2), lax.div(z, 4)
    partner = me + (3 - 2 * x) * 16
    my_slot = x_low * 16 + z * 2 + core
    row_class = x_low * 2 + z_high
    col_class = lax.rem(z, 4) * 2 + core

    loads = [
        pltpu.make_async_copy(source, target, load_sem.at[n])
        for n, (source, target) in enumerate(
            (
                (labels_hbm, labels),
                (u_hbm, right),
                (l_hbm.at[:, pl.ds(0, FIRST), :], left_first),
                (child_hbm.at[:, pl.ds(0, FIRST), :], child_first),
                (l_hbm, left),
                (child_hbm, child),
                (entries_hbm, front),
            )
        )
    ]
    for load in loads[:4]:
        load.start()

    to_core = [core, 1 - core]
    base = [[(side * 2 + xl) * 16 + to_core[fc] for fc in range(2)] for xl in range(2)]

    barrier = pltpu.get_barrier_semaphore()

    def signal(semaphore, device):
        pl.semaphore_signal(semaphore, inc=1, device_id={"dev": device}, device_id_type=MESH)

    def along(step):
        return lax.rem(z + step + 8, 8) * 2

    mine = (side * 2 + x_low) * 16 + core
    others = [
        (side * 2 + x_low) * 16 + 1 - core,
        (side * 2 + 1 - x_low) * 16 + core,
        (side * 2 + 1 - x_low) * 16 + 1 - core,
    ]
    for step in (1, -1):
        for column in others[::-1] + [mine]:
            signal(barrier, column + along(step))
    signal(barrier, partner)
    for column in others:
        signal(barrier, column + z * 2)
    for load in loads[4:6]:
        load.start()

    loads[0].wait()
    row_classes = [lax.rem(labels[side, row_class + 4 * k], 8) for k in range(8)]
    for c in range(8):
        at = jnp.int32(0)
        for k in range(1, 8):
            at = jnp.where(row_classes[k] == c, k, at)
        row_at[c] = at
    own_classes = [lax.rem(labels[side, col_class + 8 * m], 8) for m in range(4)]
    other_classes = [lax.rem(labels[1 - side, col_class + 8 * m], 8) for m in range(4)]
    for c in range(8):
        at = jnp.int32(-1)
        for m in range(4):
            at = jnp.where(own_classes[m] == c, m, at)
        own_at[c] = at
        at = jnp.int32(0)
        for m in range(1, 4):
            at = jnp.where(other_classes[m] == c, m, at)
        other_at[c] = at

    loads[1].wait()
    right_hi[...], right_lo[...] = split(right[...])
    loads[2].wait()
    loads[3].wait()

    def multiply(rows, columns):
        high, low = split(rows)
        hi_columns = right_hi[:, columns]
        product = jnp.dot(high, hi_columns, preferred_element_type=F32)
        product += jnp.dot(low, hi_columns, preferred_element_type=F32)
        return product + jnp.dot(high, right_lo[:, columns], preferred_element_type=F32)

    classes = [n % 2 * 2 + n // 2 for n in range(4)]
    at = [row_at[(1 - side) * 4 + c] for c in classes] + [row_at[side * 4 + c] for c in classes]
    rows = jnp.concatenate([left_first[k] for k in at], axis=0)
    for half in range(2):
        product = multiply(rows, pl.ds(half * 256, 256))
        for n, k in enumerate(at):
            for part in range(2):
                m = 2 * half + part
                tile = product[n * FIRST : (n + 1) * FIRST, part * TILE : (part + 1) * TILE]
                tile = child_first[k * 4 + m] - tile
                if n < 4:
                    outgoing_first[n * 4 + m] = tile
                else:
                    for first, count in CHUNKS[:EARLY]:
                        own[0 if first == 0 else 1][(n - 4) * 4 + m] = tile[first : first + count]
    pl.semaphore_wait(barrier, 12)

    swaps = []
    for n, (first, count) in enumerate(CHUNKS):
        source = outgoing_first if n < EARLY else outgoing
        for piece in range(4):
            tiles = pl.ds(piece * 4, 4)
            swaps.append(
                pltpu.make_async_remote_copy(
                    src_ref=source.at[tiles, pl.ds(first, count), :],
                    dst_ref=swapped[4 * n + piece],
                    send_sem=swap_send.at[4 * n + piece],
                    recv_sem=swap_recv.at[4 * n + piece],
                    device_id={"dev": partner},
                    device_id_type=MESH,
                )
            )
    for swap in swaps[: 4 * EARLY]:
        swap.start()
    for step in (1, -1):
        signal(known_sem.at[0], mine + along(step))

    loads[4].wait()
    loads[5].wait()
    pl.semaphore_wait(known_sem.at[0], 2)
    for step in (2, -2):
        signal(known_sem.at[1], mine + along(step))

    def update(c, put):
        ks = [row_at[c], row_at[c + 2]]
        rows = jnp.concatenate([left[k] for k in ks], axis=0)
        for half in range(2):
            product = multiply(rows, pl.ds(half * 256, 256))
            for n, k in enumerate(ks):
                for part in range(2):
                    m = 2 * half + part
                    tile = product[n * TILE : (n + 1) * TILE, part * TILE : (part + 1) * TILE]
                    put(n, m, child[k * 4 + m] - tile)

    def other_step(pair, carry):
        def put(n, m, tile):
            outgoing[(pair * 2 + n) * 4 + m] = tile

        update((1 - side) * 4 + pair, put)
        return carry

    def own_step(pair, carry):
        def put(n, m, tile):
            for part, (first, count) in list(zip(own, CHUNKS))[EARLY:]:
                part[(pair * 2 + n) * 4 + m] = tile[first : first + count]

        update(side * 4 + pair, put)
        return carry

    lax.fori_loop(0, 2, other_step, 0)
    for swap in swaps[4 * EARLY :]:
        swap.start()
    loads[6].start()
    pl.semaphore_wait(known_sem.at[1], 2)

    for n, (first, count) in enumerate(CHUNKS):
        rows = pl.ds(first, count)
        received[n][ZERO] = jnp.zeros((count, TILE), F32)
        if n == 1:
            lax.fori_loop(0, 2, own_step, 0)

        for pieces in ((0,), (1,), (2,), (3,)) if n < APART else ((0, 1), (2, 3)):
            half = pieces[0] // 2
            order = ORDERS[n][half]

            def pick(to_z, fc, piece, n=n):
                c = lax.rem(to_z, 4) * 2 + to_core[fc]
                mine, other = own_at[c], other_at[c]
                here = own[n][piece * 4 + jnp.maximum(mine, 0)]
                there = swapped[4 * n + piece][other]
                return jnp.where(mine >= 0, here, there)

            def pack(to_z, rows=rows, pick=pick, pieces=pieces):
                for piece in pieces:
                    for fc in range(2):
                        packed[to_z * 4 + piece % 2 * 2 + fc, rows, :] = pick(to_z, fc, piece)

            def send_direct(to_z, n=n, rows=rows, pieces=pieces):
                for piece in pieces:
                    xl = piece % 2
                    for fc in range(2):

                        def start(fc=fc, xl=xl):
                            pltpu.make_async_remote_copy(
                                src_ref=packed.at[to_z * 4 + xl * 2 + fc, rows, :],
                                dst_ref=received[n].at[my_slot],
                                send_sem=send_sem.at[n],
                                recv_sem=recv_sem.at[n],
                                device_id={"dev": base[xl][fc] + to_z * 2},
                                device_id_type=MESH,
                            ).start()

                        if fc:
                            start()
                        else:
                            pl.when((to_z != z) | (x_low != xl))(start)

            def send_indirect(to_z, via, rows=rows, n=n):
                pltpu.make_async_remote_copy(
                    src_ref=packed.at[pl.ds(to_z * 4, 4), rows, :],
                    dst_ref=passing,
                    send_sem=send_sem.at[n],
                    recv_sem=pass_sem.at[0],
                    device_id={"dev": mine + via * 2},
                    device_id_type=MESH,
                ).start()

            def send(to_z, n=n, direct=send_direct, indirect=send_indirect):
                detour = [d for d in DETOURS if d[2] == to_z] if n == RELAY else []
                if detour:
                    from_z, via, _ = detour[0]
                    pl.when(z == from_z)(lambda: indirect(to_z, via))
                    pl.when(z != from_z)(lambda: direct(to_z))
                else:
                    direct(to_z)

            for piece in pieces:
                swaps[4 * n + piece].wait_recv()
            pack(order[0])
            for to_z, next_z in zip(order, order[1:]):
                pack(next_z)
                send(to_z)
            for piece in pieces:

                def keep(n=n, pick=pick, piece=piece):
                    received[n][my_slot] = pick(z, 0, piece)

                pl.when((z_high == half) & (x_low == piece % 2))(keep)
            send(order[-1])

        if n == RELAY + 1:

            def forward(from_z, to_z):
                pltpu.make_async_copy(passing, passing, pass_sem.at[0]).wait()
                for xl in range(2):
                    for fc in range(2):
                        pltpu.make_async_remote_copy(
                            src_ref=passing.at[xl * 2 + fc],
                            dst_ref=received[RELAY].at[x_low * 16 + from_z * 2 + core],
                            send_sem=pass_sem.at[1],
                            recv_sem=recv_sem.at[RELAY],
                            device_id={"dev": base[xl][fc] + to_z * 2},
                            device_id_type=MESH,
                        ).start()

            for from_z, via, to_z in DETOURS:
                pl.when(z == via)(lambda from_z=from_z, to_z=to_z: forward(from_z, to_z))

    row_part = [[], []]
    col_part = [[], []]
    for c in range(2):
        for s in range(6):
            at = jnp.int32(-1)
            for i in range(32):
                x_part = jnp.where(side == c, i % 4 // 2, 1 - i % 4 // 2)
                here = labels[c, i] == 8 * s + x * 2 + z_high
                at = jnp.where(here, x_part * 16 + i % 2 * 8, at)
            row_part[c].append(at)
            at = jnp.int32(-1)
            for j in range(32):
                at = jnp.where(labels[c, j] == 8 * s + col_class, j % 8, at)
            col_part[c].append(at)

    loads[6].wait()
    for n, (first, count) in enumerate(CHUNKS):
        rows = pl.ds(first, count)
        arrived = received[n].at[pl.ds(0, OWNERS - 1)]
        pltpu.make_async_copy(arrived, arrived, recv_sem.at[n]).wait()
        for slot in range(36):
            total = front[slot, rows, :]
            for c in range(2):
                r, q = row_part[c][slot // 6], col_part[c][slot % 6]
                total += received[n][jnp.where((r >= 0) & (q >= 0), r + q, ZERO)]
            front[slot, rows, :] = total
    for _, via, _ in DETOURS:
        pl.when(z == via)(lambda: pltpu.make_async_copy(passing, passing, pass_sem.at[1]).wait())
    for swap in swaps:
        swap.wait_send()
    for n, (first, count) in enumerate(CHUNKS):
        sent = packed.at[pl.ds(0, OWNERS - 1), pl.ds(first, count), :]
        pltpu.make_async_copy(sent, sent, send_sem.at[n]).wait()


def body(child_tiles, l_slab, u_slab, parent_own_entries, parent_label):
    far = pl.BlockSpec(memory_space=pltpu.HBM)
    dma = pltpu.SemaphoreType.DMA
    return pl.pallas_call(
        kernel,
        name="extend_add",
        out_shape=pltpu.VMEM(parent_own_entries.shape, F32),
        in_specs=[far] * 5,
        out_specs=pl.BlockSpec(memory_space=pltpu.VMEM),
        scratch_shapes=[
            pltpu.VMEM((32, TILE, TILE), F32),
            pltpu.VMEM((32, FIRST, TILE), F32),
            pltpu.VMEM((8, TILE, 512), F32),
            pltpu.VMEM((8, FIRST, 512), F32),
            pltpu.VMEM((512, 512), F32),
            pltpu.VMEM((512, 512), BF16),
            pltpu.VMEM((512, 512), BF16),
            pltpu.VMEM((16, FIRST, TILE), F32),
            pltpu.VMEM((16, TILE, TILE), F32),
            pltpu.VMEM((OWNERS, TILE, TILE), F32),
            *[pltpu.VMEM((OWNERS + 1, count, TILE), F32) for _, count in CHUNKS],
            *[pltpu.VMEM((16, count, TILE), F32) for _, count in CHUNKS],
            *[pltpu.VMEM((4, count, TILE), F32) for _, count in CHUNKS for _ in range(4)],
            pltpu.SMEM((2, 32), jnp.int32),
            pltpu.SMEM((8,), jnp.int32),
            pltpu.SMEM((8,), jnp.int32),
            pltpu.SMEM((8,), jnp.int32),
            dma((7,)),
            pltpu.SemaphoreType.REGULAR((2,)),
            dma((4 * NCH,)),
            dma((4 * NCH,)),
            dma((NCH,)),
            dma((NCH,)),
            pltpu.VMEM((4, CHUNKS[RELAY][1], TILE), F32),
            dma((2,)),
        ],
        compiler_params=pltpu.CompilerParams(
            collective_id=0, has_side_effects=True, vmem_limit_bytes=40 * 2**20
        ),
    )(
        *[
            pltpu.with_memory_space_constraint(array, pltpu.HBM)
            for array in (
                parent_label,
                child_tiles,
                l_slab.reshape(8, TILE, 512),
                u_slab,
                parent_own_entries,
            )
        ]
    )


def solution(mesh):
    in_specs = (
        P(("sub", "dev"), None, None),
        P(("sub", "dev"), None),
        P(None, ("sub", "dev")),
        P(("sub", "dev"), None, None),
        P("sub", None),
    )
    out_specs = P(("sub", "dev"), None, None)
    return jax.shard_map(body, mesh=mesh, in_specs=in_specs, out_specs=out_specs, check_vma=False)
```
